32 devices in a mesh: groups: 2 (over x), row: 16 (over z, y, core).
Axes of the slice: x: 2, y: 2, z: 4, core: 2. Of those that a mesh axis runs over, the one named last changes fastest.
Arguments:
- elevation: float32 [512, 8192], P(('groups', 'row')), parts along dimension 0, may hold values from -2048 to 4096
- bin_index: int32 [512, 8192], P(('groups', 'row')), parts along dimension 0, may hold values from 0 to 1023, as said below
- ranks: int32 [4], P('groups'), parts along dimension 0, may hold values from 20971 to 2076128, as said below
Outputs:
- shaded: float32 [512, 8192], P(('groups', 'row')), parts along dimension 0
The draws below stay inside these ranges and needn't reach their ends.
There are 2 independent parts, one for each index of `groups`. The reference program is written for one: setup_inputs(seed, part) draws one part's arguments, and reference() takes and returns one part's arrays. A program takes and returns all parts, laid end to end along the dimension named above; each array names one. Nothing has to cross between parts.
Inputs may be any that keep to these rules, and one draw needn't show every extreme that they name: The bins have fixed edges: a cell with 0 < bin_index < 1023 has an elevation at or above 2 bin_index and below 2 bin_index + 2; bin 0 holds every elevation below 2 and bin 1024 - 1 every elevation at or above 2046. `ranks`: the first entry lies below 104857 and the second at or above 1992245.
All inputs are finite; a program needn't handle non-finite values.
Results may differ from the reference program's by a relative error of at most 0.0049.
Values sent between devices are 32-bit elements; how exact they have to be, the bound alone decides.
A program may use at most 64 MiB of HBM per device.

```python
import jax
import jax.numpy as jnp
from jax import lax

COLS = 8192
BINS = 1024
NROWS = 256
TOTAL = 2097152


def relief_bins(key):
    subkeys = jax.random.split(key, 6)
    amplitude = jax.random.randint(subkeys[0], (), BINS // 4, BINS * 3 // 4, jnp.int32)
    offset = jax.random.randint(subkeys[1], (), 0, BINS - amplitude - 64, jnp.int32)
    curvature = jax.random.randint(subkeys[2], (), -(BINS // 8), BINS // 8 + 1, jnp.int32)
    column_tilt = jax.random.randint(subkeys[3], (), 0, 48, jnp.int32)
    reversed_trend = jax.random.randint(subkeys[4], (), 0, 2, jnp.int32)
    roughness = jax.random.randint(subkeys[5], (NROWS, COLS), -6, 7, jnp.int32)
    row_fraction = jnp.arange(NROWS, dtype=jnp.int32) * 1024 // NROWS
    row_trend = jnp.where(reversed_trend == 1, 1023 - row_fraction, row_fraction)
    row_term = amplitude * row_trend // 1024 + curvature * row_trend * (1023 - row_trend) // 262144
    column_fraction = jnp.arange(COLS, dtype=jnp.int32) * 1024 // COLS
    column_term = column_tilt * column_fraction // 1024
    field = offset + 32 + row_term[:, None] + column_term[None, :] + roughness
    lowest = jnp.min(field)
    spread = jnp.maximum(jnp.max(field) - lowest, 1)
    scaled = (field - lowest) * (BINS + 76) // spread - 38
    return jnp.clip(scaled, 0, BINS - 1).astype(jnp.int32)


def draw_bin_index(key, part):
    return relief_bins(jax.random.fold_in(key, 7))


def draw_elevation(key, part):
    bin_field = relief_bins(jax.random.fold_in(key, 7))
    offset_key = jax.random.fold_in(key, 8)
    excess_keys = jax.random.split(jax.random.fold_in(key, 9), 3)
    top_extent = jax.random.uniform(excess_keys[0], (), jnp.float32, BINS * 0.5, BINS * 2.0)
    bottom_extent = jax.random.uniform(excess_keys[1], (), jnp.float32, BINS * 0.5, BINS * 2.0)
    unit = jax.random.uniform(excess_keys[2], (NROWS, COLS), jnp.float32, 0.0, 0.999)
    fraction = 0.5 + 0.15 * jax.random.truncated_normal(offset_key, -3.2, 3.2, (NROWS, COLS), jnp.float32)
    profile = unit * unit
    base = 2.0 * (bin_field.astype(jnp.float32) + fraction)
    raised = jnp.where(bin_field == BINS - 1, top_extent * profile, 0.0)
    lowered = jnp.where(bin_field == 0, bottom_extent * profile, 0.0)
    return base + raised - lowered


def draw_ranks(key, part):
    first, second = jax.random.split(key, 2)
    lower = jax.random.randint(first, (1,), TOTAL // 100, TOTAL // 20, jnp.int32)
    upper = jax.random.randint(second, (1,), TOTAL // 100 * 95, TOTAL // 100 * 99, jnp.int32)
    return jnp.concatenate([lower, upper])


def setup_inputs(seed: int = 0, part: int = 0) -> dict:
    splits = jax.random.split(jax.random.key(seed), 4)
    part_splits = jax.random.split(jax.random.fold_in(splits[3], part), 4)
    elevation = draw_elevation(jax.random.fold_in(jax.random.fold_in(splits[3], part), 71), part)
    bin_index = draw_bin_index(jax.random.fold_in(jax.random.fold_in(splits[3], part), 71), part)
    ranks = draw_ranks(jax.random.fold_in(jax.random.fold_in(splits[3], part), 71), part)
    return dict(elevation=elevation, bin_index=bin_index, ranks=ranks)


binomial = (1.0 / 64, 6.0 / 64, 15.0 / 64, 20.0 / 64, 15.0 / 64, 6.0 / 64, 1.0 / 64)
zfactor = 200.0
cos_zenith = 0.70710678
sin_zenith = 0.70710678
light_x = -0.70710678
light_y = 0.70710678

def filter_cols(padded):
    width = padded.shape[1] - 6
    total = binomial[0] * padded[:, 0:width]
    for offset in range(1, 7):
        total = total + binomial[offset] * padded[:, offset:offset + width]
    return total

def filter_rows(padded):
    height = padded.shape[0] - 6
    total = binomial[0] * padded[0:height, :]
    for offset in range(1, 7):
        total = total + binomial[offset] * padded[offset:offset + height, :]
    return total

def shade(smooth, span):
    height = smooth.shape[0] - 2
    width = smooth.shape[1] - 2

    def window(drow, dcol):
        return smooth[drow:drow + height, dcol:dcol + width]
    east = window(0, 2) + 2.0 * window(1, 2) + window(2, 2)
    west = window(0, 0) + 2.0 * window(1, 0) + window(2, 0)
    south = window(2, 0) + 2.0 * window(2, 1) + window(2, 2)
    north = window(0, 0) + 2.0 * window(0, 1) + window(0, 2)
    scale = zfactor / (8.0 * span)
    grad_x = (east - west) * scale
    grad_y = (south - north) * scale
    light = (cos_zenith - sin_zenith * (light_x * grad_x + light_y * grad_y)) * lax.rsqrt(1.0 + grad_x * grad_x + grad_y * grad_y)
    return jnp.maximum(light, 0.0)

def reference(elevation, bin_index, ranks):
    counts = jnp.zeros((BINS,), jnp.float32).at[bin_index.reshape(-1)].add(1.0)
    span = jnp.max(elevation) - jnp.min(elevation)
    cumulative = jnp.cumsum(counts.astype(jnp.int32), dtype=jnp.int32)
    table = jnp.clip((cumulative - ranks[0]).astype(jnp.float32) / (ranks[1] - ranks[0]).astype(jnp.float32), 0.0, 1.0).astype(jnp.bfloat16)
    stretch = table.astype(jnp.float32)[bin_index]
    padded = jnp.pad(elevation, 4)
    smooth = filter_rows(filter_cols(padded))
    light = shade(smooth, span)
    return stretch * (0.5 + light)
```

```python
import functools

import jax
import jax.numpy as jnp
from jax import lax
from jax.experimental import pallas as pl
from jax.experimental.pallas import tpu as pltpu
from jax.sharding import PartitionSpec as P

BINS = 1024
zfactor = 200.0
cos_zenith = 0.70710678
sin_zenith = 0.70710678
light_x = -0.70710678
light_y = 0.70710678
LANES = 128
HALO = 4
PAD = 128
SMOOTH = (1.0, 8.0, 28.0, 56.0, 70.0, 56.0, 28.0, 8.0, 1.0)
SLOPE = (-1.0, -6.0, -14.0, -14.0, 0.0, 14.0, 14.0, 6.0, 1.0)
UPPER = 32
LOWER = BINS // UPPER
LEVELS = 1023.0
FIELD = 10
PIECES = 4
MESH = pl.DeviceIdType.MESH


def band(first):
    row = lax.broadcasted_iota(jnp.int32, (LANES, LANES), 0)
    col = lax.broadcasted_iota(jnp.int32, (LANES, LANES), 1)
    delta = row + first - col
    rise = jnp.zeros(row.shape, jnp.float32)
    level = jnp.zeros(row.shape, jnp.float32)
    for k in range(9):
        here = delta == k - HALO
        rise = jnp.where(here, SLOPE[k], rise)
        level = jnp.where(here, SMOOTH[k], level)
    return jnp.concatenate([rise, level], axis=1).astype(jnp.bfloat16)


def windows(parts, tiles):
    rows = []
    for t in range(tiles):
        for part in parts:
            rows.append(part[:, t * LANES : (t + 3) * LANES])
    return jnp.concatenate(rows, axis=0)


def partner(n, me, k):
    if n & (n - 1) == 0:
        return lax.bitwise_xor(me, n - k)
    return lax.rem(me + k, n)


def kernel(n, chunk, bins_hbm, elev_hbm, ranks_hbm, sums_ref, index_ref, slope_x, slope_y, bins, cells, halo, col_x, col_y,
           weights, send, recv, ranks, bins_sem, elev_sem, rank_sem, halo_send, halo_recv, send_sem, recv_sem):
    me = lax.axis_index("row")
    height, width = elev_hbm.shape
    chunks = width // chunk
    tiles = chunk // LANES
    inner = pl.ds(PAD, width)
    parts = halo_recv.shape[1]
    piece = width // parts

    def bins_load(half):
        where = (slice(None), pl.ds(pl.multiple_of(half * (width // 2), width // 2), width // 2))
        return pltpu.make_async_copy(bins_hbm.at[where], bins.at[where], bins_sem.at[half])

    elev_load = pltpu.make_async_copy(elev_hbm, cells.at[:, inner], elev_sem)
    rank_load = pltpu.make_async_copy(ranks_hbm, ranks, rank_sem)
    bins_load(0).start()
    bins_load(1).start()
    elev_load.start()
    rank_load.start()

    barrier = pltpu.get_barrier_semaphore()

    def greet(k, carry):
        pl.semaphore_signal(barrier, inc=1, device_id={"row": partner(n, me, k)}, device_id_type=MESH)
        return carry

    lax.fori_loop(1, n, greet, 0)

    for edge in (0, PAD + width):
        cells[:, pl.ds(edge, PAD)] = jnp.zeros((height, PAD), jnp.float32)
        halo[:, pl.ds(edge, PAD)] = jnp.zeros((8, PAD), jnp.float32)

    @pl.when(me == 0)
    def _():
        halo[4:8, inner] = jnp.zeros((4, width), jnp.float32)

    @pl.when(me == n - 1)
    def _():
        halo[0:4, inner] = jnp.zeros((4, width), jnp.float32)

    def halo_copy(way, p):
        rows = pl.ds(0, HALO) if way else pl.ds(height - HALO, HALO)
        cols = pl.ds(PAD + p * piece, piece)
        return pltpu.make_async_remote_copy(
            src_ref=cells.at[rows, cols], dst_ref=halo.at[pl.ds(0 if way else 4, HALO), cols],
            send_sem=halo_send.at[way, p], recv_sem=halo_recv.at[way, p],
            device_id={"row": lax.rem(me + n - 1, n) if way else lax.rem(me + 1, n)}, device_id_type=MESH)

    urow = lax.broadcasted_iota(jnp.int32, (UPPER, chunk), 0)
    upper_iota = (4 * lax.rem(urow, 8) + urow // 8).astype(jnp.float32).astype(jnp.bfloat16)
    lower_iota = lax.broadcasted_iota(jnp.int32, (LOWER, chunk), 0).astype(jnp.float32).astype(jnp.bfloat16)
    one, zero = jnp.ones((), jnp.bfloat16), jnp.zeros((), jnp.bfloat16)

    def count(i, total):
        whole = bins[:, pl.ds(pl.multiple_of(i * chunk, chunk), chunk)]
        high = (whole >> 5).astype(jnp.float32)
        low = (whole & 31).astype(jnp.float32)
        for r in range(height):
            hot_u = jnp.where(jnp.broadcast_to(high[r : r + 1], (UPPER, chunk)).astype(jnp.bfloat16) == upper_iota, one, zero)
            hot_l = jnp.where(jnp.broadcast_to(low[r : r + 1], (LOWER, chunk)).astype(jnp.bfloat16) == lower_iota, one, zero)
            total = total + lax.dot_general(hot_u, hot_l, (((1,), (1,)), ((), ())),
                                            preferred_element_type=jnp.float32)
        return total

    def half_count(half, total):
        bins_load(half).wait()
        for i in range(chunks // 2):
            total = count(half * (chunks // 2) + i, total)

        @pl.when(half == 0)
        def _():
            elev_load.wait()
            pl.semaphore_wait(barrier, n - 1)

            @pl.when(me < n - 1)
            def _():
                for p in range(parts):
                    halo_copy(0, p).start()

            @pl.when(me > 0)
            def _():
                for p in range(parts):
                    halo_copy(1, p).start()

        return total

    total = lax.fori_loop(0, 2, half_count, jnp.zeros((UPPER, LOWER), jnp.float32))
    tops, bottoms = [], []
    for c in range(width // LANES):
        for r in range(height // 8):
            block = cells[8 * r : 8 * r + 8, PAD + c * LANES : PAD + (c + 1) * LANES]
            if len(tops) < 4:
                tops.append(block)
                bottoms.append(block)
            else:
                at = (c * (height // 8) + r) % 4
                tops[at] = jnp.maximum(tops[at], block)
                bottoms[at] = jnp.minimum(bottoms[at], block)
    top = functools.reduce(jnp.maximum, tops)
    bottom = functools.reduce(jnp.minimum, bottoms)
    counts = jnp.concatenate([total[8 * q : 8 * q + 8] for q in range(UPPER // 8)], axis=1)
    send[0:8, :] = counts
    send[8:9, :] = jnp.max(top, axis=0, keepdims=True)
    send[9:10, :] = jnp.max(-bottom, axis=0, keepdims=True)

    def post(k, carry):
        pltpu.make_async_remote_copy(
            src_ref=send, dst_ref=recv.at[k], send_sem=send_sem, recv_sem=recv_sem,
            device_id={"row": partner(n, me, k)}, device_id_type=MESH).start()
        return carry

    lax.fori_loop(1, n, post, 0)

    for k in range(3):
        weights[k * LANES : (k + 1) * LANES, :] = band((k - 1) * LANES)
    middle = cells[0:1, PAD : PAD + 1]

    def split(x):
        x = x - middle
        first = x.astype(jnp.bfloat16).astype(jnp.float32)
        return first, x - first

    def own_rows(i, carry):
        at = pl.multiple_of(i * chunk, chunk)
        first, rest = split(cells[:, pl.ds(at, chunk + 2 * PAD)])
        got = jnp.dot(windows((first.astype(jnp.bfloat16), rest.astype(jnp.bfloat16)), tiles), weights[...],
                      preferred_element_type=jnp.float32)
        for t in range(tiles):
            both = got[2 * height * t : 2 * height * t + height] + got[2 * height * t + height : 2 * height * (t + 1)]
            col_x[i * tiles + t, 8 : 8 + height, :] = both[:, 0:LANES]
            col_y[i * tiles + t, 8 : 8 + height, :] = both[:, LANES : 2 * LANES]
        whole = bins[:, pl.ds(at, chunk)]
        group = whole >> 7
        third = jnp.where(group >= 6, 2, jnp.where(group >= 3, 1, 0))
        shift = FIELD * (group - 3 * third)
        index_ref[:, pl.ds(at, chunk)] = (third << 12) + (shift << 7) + (whole & (LANES - 1))
        return carry

    lax.fori_loop(0, chunks, own_rows, 0, unroll=4)

    def halo_rows(i):
        at = i * chunk
        first, rest = split(halo[:, pl.ds(at, chunk + 2 * PAD)])
        pair = jnp.concatenate([first, rest], axis=0).astype(jnp.bfloat16)
        got = jnp.dot(windows((pair,), tiles), weights[...], preferred_element_type=jnp.float32)
        for t in range(tiles):
            both = got[16 * t : 16 * t + 8] + got[16 * t + 8 : 16 * t + 16]
            for col, lanes in ((col_x, slice(0, LANES)), (col_y, slice(LANES, 2 * LANES))):
                col[i * tiles + t, 0:8, :] = both[:, lanes]
                col[i * tiles + t, 8 + height : 16 + height, :] = both[:, lanes]

    def down_rows(t):
        for r in range(height // 8):
            rows = [col_x[t, 8 * r + 4 + k : 8 * r + 12 + k, :] for k in range(9)]
            out = SMOOTH[4] * rows[4] + (rows[0] + rows[8])
            for k in range(1, 4):
                out = out + SMOOTH[k] * (rows[k] + rows[8 - k])
            slope_x[8 * r : 8 * r + 8, t * LANES : (t + 1) * LANES] = out
            rows = [col_y[t, 8 * r + 4 + k : 8 * r + 12 + k, :] if k != 4 else None for k in range(9)]
            out = 14.0 * ((rows[5] - rows[3]) + (rows[6] - rows[2])) + 6.0 * (rows[7] - rows[1]) + (rows[8] - rows[0])
            slope_y[8 * r : 8 * r + 8, t * LANES : (t + 1) * LANES] = out

    def arrive(p):
        @pl.when(me > 0)
        def _():
            halo_copy(0, p).wait_recv()

        @pl.when(me < n - 1)
        def _():
            halo_copy(1, p).wait_recv()

    arrive(0)
    each = chunks // parts
    for p in range(parts):
        if p + 1 < parts:
            arrive(p + 1)
        for i in range(p * each, (p + 1) * each):
            halo_rows(i)
        for t in range(p * each * tiles, (p + 1) * each * tiles):
            down_rows(t)

    rank_load.wait()
    everything = pltpu.make_async_copy(recv.at[pl.ds(1, n - 1)], recv.at[pl.ds(1, n - 1)], recv_sem)
    everything.wait()

    def take(k, carry):
        return carry[0] + recv[k, 0:8, :], jnp.maximum(carry[1], recv[k, 8:10, :])

    counts, ends = lax.fori_loop(1, n, take, (send[0:8, :], send[8:10, :]), unroll=n <= 16)
    sums_ref[0:8, :] = counts
    sums_ref[8:10, :] = ends
    sums_ref[10:11, :] = jnp.full((1, LANES), ranks[0], jnp.int32).astype(jnp.float32)
    sums_ref[11:12, :] = jnp.full((1, LANES), ranks[1], jnp.int32).astype(jnp.float32)

    @pl.when(me < n - 1)
    def _():
        for p in range(parts):
            halo_copy(0, p).wait_send()

    @pl.when(me > 0)
    def _():
        for p in range(parts):
            halo_copy(1, p).wait_send()

    pltpu.make_async_copy(recv.at[pl.ds(1, n - 1)], recv.at[pl.ds(1, n - 1)], send_sem).wait()


def shade_kernel(chunk, sums_ref, index_ref, slope_x, slope_y, out_ref, result, out_sem):
    height, width = index_ref.shape
    chunks = width // chunk

    counts = sums_ref[0:8, :]
    ends = jnp.max(sums_ref[8:10, :], axis=1, keepdims=True)
    span = ends[0:1] + ends[1:2]
    scale = jnp.broadcast_to(zfactor / (8.0 * span) * (1.0 / 4096.0), (8, LANES))
    whole = counts.astype(jnp.int32)
    lane_in = lax.broadcasted_iota(jnp.int32, (LANES, LANES), 0)
    lane_out = lax.broadcasted_iota(jnp.int32, (LANES, LANES), 1)
    triangle = jnp.where(lane_in <= lane_out, 1.0, 0.0).astype(jnp.bfloat16)
    digits = jnp.concatenate([(whole & 255), ((whole >> 8) & 255), (whole >> 16), jnp.zeros_like(whole)],
                             axis=0).astype(jnp.float32).astype(jnp.bfloat16)
    sums = jnp.dot(digits, triangle, preferred_element_type=jnp.float32)
    within = sums[0:8] + 256.0 * sums[8:16] + 65536.0 * sums[16:24]
    before = jnp.zeros((1, 1), jnp.float32)
    rows = []
    for b in range(8):
        rows.append(before)
        before = before + within[b : b + 1, LANES - 1 : LANES]
    cumulative = (within + jnp.concatenate(rows, axis=0)).astype(jnp.int32)
    first = jnp.broadcast_to(sums_ref[10:11, :], (8, LANES)).astype(jnp.int32)
    second = jnp.broadcast_to(sums_ref[11:12, :], (8, LANES)).astype(jnp.int32)
    table = jnp.clip((cumulative - first).astype(jnp.float32) / (second - first).astype(jnp.float32), 0.0, 1.0)
    fixed = jnp.floor(table * LEVELS + 0.5).astype(jnp.int32)
    spread = [jnp.broadcast_to(fixed[b : b + 1], (8, LANES)) for b in range(8)]
    words = [spread[0] + (spread[1] << FIELD) + (spread[2] << (2 * FIELD)),
             spread[3] + (spread[4] << FIELD) + (spread[5] << (2 * FIELD)),
             spread[6] + (spread[7] << FIELD)]

    def out_copy(i):
        at = pl.multiple_of(i * chunk, chunk)
        where = (slice(None), pl.ds(at, chunk))
        return pltpu.make_async_copy(result.at[where], out_ref.at[where], out_sem.at[i])

    def finish(i, carry):
        at = pl.multiple_of(i * chunk, chunk)
        for r in range(height // 8):
            for c in range(chunk // LANES):
                rows = pl.ds(8 * r, 8)
                cols = pl.ds(at + c * LANES, LANES)
                which = index_ref[rows, cols]
                lane = which & (LANES - 1)
                word = jnp.take_along_axis(words[0], lane, axis=1)
                word = jnp.where(which >= 4096, jnp.take_along_axis(words[1], lane, axis=1), word)
                word = jnp.where(which >= 8192, jnp.take_along_axis(words[2], lane, axis=1), word)
                stretch = ((word >> ((which >> 7) & 31)) & 1023).astype(jnp.float32)
                gx = slope_x[rows, cols] * scale
                gy = slope_y[rows, cols] * scale
                light = (cos_zenith - sin_zenith * (light_x * gx + light_y * gy)) * lax.rsqrt(
                    1.0 + gx * gx + gy * gy)
                result[rows, cols] = stretch * (0.5 / LEVELS + (1.0 / LEVELS) * jnp.maximum(light, 0.0))
        out_copy(i).start()
        return carry

    lax.fori_loop(0, chunks, finish, 0)

    def flush(i, carry):
        out_copy(i).wait()
        return carry

    lax.fori_loop(0, chunks, flush, 0)


def chunk_of(width):
    chunk = 1024
    while width % chunk:
        chunk //= 2
    return chunk


def solution(mesh):
    n = mesh.shape["row"]

    def body(elevation, bin_index, ranks):
        height, width = elevation.shape
        chunk = chunk_of(width)
        chunks = width // chunk
        grid = (height, width)
        room = 24 << 20
        block = pltpu.VMEM(grid, jnp.float32)
        whole = jax.ShapeDtypeStruct(grid, jnp.float32)
        anywhere = pl.BlockSpec(memory_space=pl.ANY)
        inside = pl.BlockSpec(memory_space=pltpu.VMEM)
        wide = width + 2 * PAD
        sums, index, slope_x, slope_y = pl.pallas_call(
            functools.partial(kernel, n, chunk),
            out_shape=[jax.ShapeDtypeStruct((16, LANES), jnp.float32), jax.ShapeDtypeStruct(grid, jnp.int32), whole, whole],
            in_specs=[anywhere] * 3,
            out_specs=[inside] * 4,
            scratch_shapes=[
                pltpu.VMEM(grid, jnp.int32),
                pltpu.VMEM((height, wide), jnp.float32),
                pltpu.VMEM((8, wide), jnp.float32),
                pltpu.VMEM((width // LANES, height + 16, LANES), jnp.float32),
                pltpu.VMEM((width // LANES, height + 16, LANES), jnp.float32),
                pltpu.VMEM((3 * LANES, 2 * LANES), jnp.bfloat16),
                pltpu.VMEM((10, LANES), jnp.float32),
                pltpu.VMEM((n, 10, LANES), jnp.float32),
                pltpu.SMEM((2,), jnp.int32),
                pltpu.SemaphoreType.DMA((2,)),
                pltpu.SemaphoreType.DMA,
                pltpu.SemaphoreType.DMA,
                pltpu.SemaphoreType.DMA((2, PIECES)),
                pltpu.SemaphoreType.DMA((2, PIECES)),
                pltpu.SemaphoreType.DMA,
                pltpu.SemaphoreType.DMA,
            ],
            compiler_params=pltpu.CompilerParams(collective_id=0, has_side_effects=True, vmem_limit_bytes=room),
        )(*[pltpu.with_memory_space_constraint(x, pltpu.HBM) for x in (bin_index, elevation, ranks)])
        return pl.pallas_call(
            functools.partial(shade_kernel, chunk),
            out_shape=whole,
            in_specs=[inside] * 4,
            out_specs=anywhere,
            scratch_shapes=[block, pltpu.SemaphoreType.DMA((chunks,))],
            compiler_params=pltpu.CompilerParams(vmem_limit_bytes=32 * height * width * 4),
        )(sums, index, slope_x, slope_y)

    in_specs = (P(("groups", "row"), None), P(("groups", "row"), None), P("groups"))
    return jax.shard_map(body, mesh=mesh, in_specs=in_specs, out_specs=P(("groups", "row"), None), check_vma=False)
```

```python
import functools

import jax
import jax.numpy as jnp
from jax import lax
from jax.experimental import pallas as pl
from jax.experimental.pallas import tpu as pltpu
from jax.sharding import PartitionSpec as P

BINS = 1024
zfactor = 200.0
cos_zenith = 0.70710678
sin_zenith = 0.70710678
light_x = -0.70710678
light_y = 0.70710678
LANES = 128
HALO = 4
PAD = 128
SMOOTH = (1.0, 8.0, 28.0, 56.0, 70.0, 56.0, 28.0, 8.0, 1.0)
SLOPE = (-1.0, -6.0, -14.0, -14.0, 0.0, 14.0, 14.0, 6.0, 1.0)
UPPER = 32
LOWER = BINS // UPPER
LEVELS = 255.0
FIELD = 8
PIECES = 4
MESH = pl.DeviceIdType.MESH


def band(first):
    row = lax.broadcasted_iota(jnp.int32, (LANES, LANES), 0)
    col = lax.broadcasted_iota(jnp.int32, (LANES, LANES), 1)
    delta = row + first - col
    rise = jnp.zeros(row.shape, jnp.float32)
    level = jnp.zeros(row.shape, jnp.float32)
    for k in range(9):
        here = delta == k - HALO
        rise = jnp.where(here, SLOPE[k], rise)
        level = jnp.where(here, SMOOTH[k], level)
    return jnp.concatenate([rise, level], axis=1).astype(jnp.bfloat16)


def windows(parts, tiles):
    rows = []
    for t in range(tiles):
        for part in parts:
            rows.append(part[:, t * LANES : (t + 3) * LANES])
    return jnp.concatenate(rows, axis=0)


def target(me, k):
    return k - 1 + (k - 1 >= me).astype(jnp.int32)


def kernel(n, chunk, bins_hbm, elev_hbm, ranks_hbm, sums_ref, bins, slope_x, slope_y, cells, halo, col_x, col_y,
           weights, extremes, high, low, send, recv, ranks, bins_sem, elev_sem, rank_sem, halo_send, halo_recv, send_sem, recv_sem):
    me = lax.axis_index("row")
    height, width = elev_hbm.shape
    chunks = width // chunk
    tiles = chunk // LANES
    inner = pl.ds(PAD, width)
    parts = halo_recv.shape[1]
    piece = width // parts

    def bins_load(half):
        where = (slice(None), pl.ds(pl.multiple_of(half * (width // 2), width // 2), width // 2))
        return pltpu.make_async_copy(bins_hbm.at[where], bins.at[where], bins_sem.at[half])

    elev_load = pltpu.make_async_copy(elev_hbm, cells.at[:, inner], elev_sem)
    rank_load = pltpu.make_async_copy(ranks_hbm, ranks, rank_sem)
    bins_load(0).start()
    bins_load(1).start()
    elev_load.start()
    rank_load.start()

    barrier = pltpu.get_barrier_semaphore()

    def greet(k, carry):
        pl.semaphore_signal(barrier, inc=1, device_id={"row": target(me, k)}, device_id_type=MESH)
        return carry

    lax.fori_loop(1, n, greet, 0)

    for edge in (0, PAD + width):
        cells[:, pl.ds(edge, PAD)] = jnp.zeros((height, PAD), jnp.float32)
        halo[:, pl.ds(edge, PAD)] = jnp.zeros((8, PAD), jnp.float32)

    @pl.when(me == 0)
    def _():
        halo[4:8, inner] = jnp.zeros((4, width), jnp.float32)

    @pl.when(me == n - 1)
    def _():
        halo[0:4, inner] = jnp.zeros((4, width), jnp.float32)

    def halo_copy(way, p):
        rows = pl.ds(0, HALO) if way else pl.ds(height - HALO, HALO)
        cols = pl.ds(PAD + p * piece, piece)
        return pltpu.make_async_remote_copy(
            src_ref=cells.at[rows, cols], dst_ref=halo.at[pl.ds(0 if way else 4, HALO), cols],
            send_sem=halo_send.at[way], recv_sem=halo_recv.at[way, p],
            device_id={"row": lax.rem(me + n - 1, n) if way else lax.rem(me + 1, n)}, device_id_type=MESH)

    urow = lax.broadcasted_iota(jnp.int32, (UPPER, chunk), 0)
    upper_iota = (4 * lax.rem(urow, 8) + urow // 8).astype(jnp.float32).astype(jnp.bfloat16)
    lower_iota = lax.broadcasted_iota(jnp.int32, (LOWER, chunk), 0).astype(jnp.float32).astype(jnp.bfloat16)
    one, zero = jnp.ones((), jnp.bfloat16), jnp.zeros((), jnp.bfloat16)

    def spread(ref, t, r):
        row = jnp.concatenate([ref[t + c, pl.ds(r, 8, stride=0), :] for c in range(tiles)], axis=1)
        return jnp.concatenate([row] * (UPPER // 8), axis=0).astype(jnp.bfloat16)

    def count(half, i, total):
        at = pl.multiple_of((half * (chunks // 2) + i) * chunk, chunk)
        whole = bins[:, pl.ds(at, chunk)]
        for c in range(tiles):
            tile = whole[:, c * LANES : (c + 1) * LANES]
            high[i * tiles + c] = (tile >> 5).astype(jnp.float32)
            low[i * tiles + c] = (tile & 31).astype(jnp.float32)
        for r in range(height):
            hot_u = jnp.where(spread(high, i * tiles, r) <= upper_iota, one, zero).astype(jnp.float8_e4m3fn)
            hot_l = jnp.where(spread(low, i * tiles, r) <= lower_iota, one, zero).astype(jnp.float8_e4m3fn)
            total = total + lax.dot_general(hot_u, hot_l, (((1,), (1,)), ((), ())),
                                            preferred_element_type=jnp.float32)
        return total

    def reach():
        tops, bottoms = [None] * 4, [None] * 4
        for c in range(width // LANES):
            for r in range(height // 8):
                block = cells[8 * r : 8 * r + 8, PAD + c * LANES : PAD + (c + 1) * LANES]
                at = (c * (height // 8) + r) % 4
                tops[at] = block if tops[at] is None else jnp.maximum(tops[at], block)
                bottoms[at] = block if bottoms[at] is None else jnp.minimum(bottoms[at], block)
        extremes[0:8, :] = functools.reduce(jnp.maximum, [x for x in tops if x is not None])
        extremes[8:16, :] = functools.reduce(jnp.minimum, [x for x in bottoms if x is not None])

    def half_count(half, total):
        bins_load(half).wait()
        for i in range(chunks // 2):
            total = count(half, i, total)

        @pl.when(half == 0)
        def _():
            elev_load.wait()
            pl.semaphore_wait(barrier, n - 1)

            @pl.when(me < n - 1)
            def _():
                for p in range(parts):
                    halo_copy(0, p).start()

            @pl.when(me > 0)
            def _():
                for p in range(parts):
                    halo_copy(1, p).start()

            reach()

        return total

    total = lax.fori_loop(0, 2, half_count, jnp.zeros((UPPER, LOWER), jnp.float32))
    counts = jnp.concatenate([total[8 * q : 8 * q + 8] for q in range(UPPER // 8)], axis=1)
    send[0:8, :] = counts
    ends = [jnp.max(extremes[0:8, :], axis=0, keepdims=True), jnp.max(-extremes[8:16, :], axis=0, keepdims=True)]
    top, bottom = [jnp.maximum(x, pltpu.roll(x, LANES // 2, 1)) for x in ends]
    send[8:9, :] = jnp.where(lax.broadcasted_iota(jnp.int32, (1, LANES), 1) < LANES // 2, top, bottom)

    def post(k, carry):
        pltpu.make_async_remote_copy(
            src_ref=send, dst_ref=recv.at[me], send_sem=send_sem, recv_sem=recv_sem,
            device_id={"row": target(me, k)}, device_id_type=MESH).start()
        return carry

    lax.fori_loop(1, n, post, 0)

    for k in range(3):
        weights[k * LANES : (k + 1) * LANES, :] = band((k - 1) * LANES)
    middle = cells[0:1, PAD : PAD + 1]

    def split(x):
        x = x - middle
        first = x.astype(jnp.bfloat16).astype(jnp.float32)
        return first, x - first

    def own_rows(i, carry):
        at = pl.multiple_of(i * chunk, chunk)
        first, rest = split(cells[:, pl.ds(at, chunk + 2 * PAD)])
        got = jnp.dot(windows((first.astype(jnp.bfloat16), rest.astype(jnp.bfloat16)), tiles), weights[...],
                      preferred_element_type=jnp.float32)
        for t in range(tiles):
            both = got[2 * height * t : 2 * height * t + height] + got[2 * height * t + height : 2 * height * (t + 1)]
            col_x[i * tiles + t, 8 : 8 + height, :] = both[:, 0:LANES]
            col_y[i * tiles + t, 8 : 8 + height, :] = both[:, LANES : 2 * LANES]
        return carry

    lax.fori_loop(0, chunks, own_rows, 0, unroll=4)

    def halo_rows(i):
        at = i * chunk
        first, rest = split(halo[:, pl.ds(at, chunk + 2 * PAD)])
        pair = jnp.concatenate([first, rest], axis=0).astype(jnp.bfloat16)
        got = jnp.dot(windows((pair,), tiles), weights[...], preferred_element_type=jnp.float32)
        for t in range(tiles):
            both = got[16 * t : 16 * t + 8] + got[16 * t + 8 : 16 * t + 16]
            for col, lanes in ((col_x, slice(0, LANES)), (col_y, slice(LANES, 2 * LANES))):
                col[i * tiles + t, 0:8, :] = both[:, lanes]
                col[i * tiles + t, 8 + height : 16 + height, :] = both[:, lanes]

    def down_rows(t):
        for r in range(height // 8):
            rows = [col_x[t, 8 * r + 4 + k : 8 * r + 12 + k, :] for k in range(9)]
            out = SMOOTH[4] * rows[4] + (rows[0] + rows[8])
            for k in range(1, 4):
                out = out + SMOOTH[k] * (rows[k] + rows[8 - k])
            slope_x[8 * r : 8 * r + 8, t * LANES : (t + 1) * LANES] = out
            rows = [col_y[t, 8 * r + 4 + k : 8 * r + 12 + k, :] if k != 4 else None for k in range(9)]
            out = 14.0 * ((rows[5] - rows[3]) + (rows[6] - rows[2])) + 6.0 * (rows[7] - rows[1]) + (rows[8] - rows[0])
            slope_y[8 * r : 8 * r + 8, t * LANES : (t + 1) * LANES] = out

    def arrive(p):
        @pl.when(me > 0)
        def _():
            halo_copy(0, p).wait_recv()

        @pl.when(me < n - 1)
        def _():
            halo_copy(1, p).wait_recv()

    arrive(0)
    each = chunks // parts
    for p in range(parts):
        if p + 1 < parts:
            arrive(p + 1)
        for i in range(p * each, (p + 1) * each):
            halo_rows(i)
        for t in range(p * each * tiles, (p + 1) * each * tiles):
            down_rows(t)

    rank_load.wait()
    everything = pltpu.make_async_copy(recv.at[pl.ds(1, n - 1)], recv.at[pl.ds(1, n - 1)], recv_sem)
    everything.wait()

    def take(k, carry):
        return carry[0] + recv[k, 0:8, :], jnp.maximum(carry[1], recv[k, 8:9, :])

    recv[me] = send[...]
    counts, ends = lax.fori_loop(1, n, take, (recv[0, 0:8, :], recv[0, 8:9, :]), unroll=n <= 16)
    sums_ref[0:8, :] = counts
    sums_ref[8:9, :] = ends
    sums_ref[10:11, :] = jnp.full((1, LANES), ranks[0], jnp.int32).astype(jnp.float32)
    sums_ref[11:12, :] = jnp.full((1, LANES), ranks[1], jnp.int32).astype(jnp.float32)

    edge = halo.at[pl.ds(0, HALO), inner]

    @pl.when(me < n - 1)
    def _():
        pltpu.make_async_copy(edge, edge, halo_send.at[0]).wait()

    @pl.when(me > 0)
    def _():
        pltpu.make_async_copy(edge, edge, halo_send.at[1]).wait()

    pltpu.make_async_copy(recv.at[pl.ds(1, n - 1)], recv.at[pl.ds(1, n - 1)], send_sem).wait()


def shade_kernel(chunk, sums_ref, index_ref, slope_x, slope_y, out_ref, result, out_sem):
    height, width = index_ref.shape
    chunks = width // chunk

    counts = sums_ref[0:8, :]
    ends = sums_ref[8:9, :]
    span = (jnp.max(ends[:, 0 : LANES // 2], axis=1, keepdims=True)
            + jnp.max(ends[:, LANES // 2 : LANES], axis=1, keepdims=True))
    scale = jnp.broadcast_to(zfactor / (8.0 * span) * (1.0 / 4096.0), (8, LANES))
    tilt = (sin_zenith * light_y) * scale
    lane = lax.broadcasted_iota(jnp.int32, (8, LANES), 1)
    row = lax.broadcasted_iota(jnp.int32, (8, LANES), 0)
    before = pltpu.roll(counts, LOWER, 1)
    above = jnp.where(row == 0, 0.0, pltpu.roll(before, 1, 0))
    before = jnp.where(lane < LOWER, above, before)
    full = jnp.take_along_axis(before, lane | (LOWER - 1), axis=1, mode="promise_in_bounds")
    cumulative = (full + (counts - before)).astype(jnp.int32)
    first = jnp.broadcast_to(sums_ref[10:11, :], (8, LANES)).astype(jnp.int32)
    second = jnp.broadcast_to(sums_ref[11:12, :], (8, LANES)).astype(jnp.int32)
    table = jnp.clip((cumulative - first).astype(jnp.float32) / (second - first).astype(jnp.float32), 0.0, 1.0)
    fixed = jnp.floor(table * LEVELS + 0.5).astype(jnp.int32)
    spread = [jnp.broadcast_to(fixed[b : b + 1], (8, LANES)) for b in range(8)]
    words = [spread[g] + (spread[g + 1] << FIELD) + (spread[g + 2] << (2 * FIELD)) + (spread[g + 3] << (3 * FIELD))
             for g in (0, 4)]

    def out_copy(i):
        at = pl.multiple_of(i * chunk, chunk)
        where = (slice(None), pl.ds(at, chunk))
        return pltpu.make_async_copy(result.at[where], out_ref.at[where], out_sem)

    def finish(i, carry):
        at = pl.multiple_of(i * chunk, chunk)
        for r in range(height // 8):
            for c in range(chunk // LANES):
                rows = pl.ds(8 * r, 8)
                cols = pl.ds(at + c * LANES, LANES)
                which = index_ref[rows, cols]
                lane = which & (LANES - 1)
                words_at = [jnp.take_along_axis(w, lane, axis=1, mode="promise_in_bounds") for w in words]
                word = jnp.where(which >= BINS // 2, words_at[1], words_at[0])
                stretch = ((word >> ((which >> 4) & 24)) & 255).astype(jnp.float32)
                rise, fall = slope_x[rows, cols], slope_y[rows, cols]
                gx, gy = rise * scale, fall * scale
                light = (cos_zenith - tilt * (fall - rise)) * lax.rsqrt(1.0 + gx * gx + gy * gy)
                result[rows, cols] = stretch * (0.5 / LEVELS + (1.0 / LEVELS) * jnp.maximum(light, 0.0))
        out_copy(i).start()
        return carry

    lax.fori_loop(0, chunks, finish, 0, unroll=True)

    pltpu.make_async_copy(result, out_ref, out_sem).wait()


def chunk_of(width):
    chunk = 1024
    while width % chunk:
        chunk //= 2
    return chunk


def solution(mesh):
    n = mesh.shape["row"]

    def body(elevation, bin_index, ranks):
        height, width = elevation.shape
        chunk = chunk_of(width)
        grid = (height, width)
        room = 24 << 20
        block = pltpu.VMEM(grid, jnp.float32)
        whole = jax.ShapeDtypeStruct(grid, jnp.float32)
        anywhere = pl.BlockSpec(memory_space=pl.ANY)
        inside = pl.BlockSpec(memory_space=pltpu.VMEM)
        wide = width + 2 * PAD
        sums, index, slope_x, slope_y = pl.pallas_call(
            functools.partial(kernel, n, chunk),
            out_shape=[jax.ShapeDtypeStruct((16, LANES), jnp.float32), jax.ShapeDtypeStruct(grid, jnp.int32), whole, whole],
            in_specs=[anywhere] * 3,
            out_specs=[inside] * 4,
            scratch_shapes=[
                pltpu.VMEM((height, wide), jnp.float32),
                pltpu.VMEM((8, wide), jnp.float32),
                pltpu.VMEM((width // LANES, height + 16, LANES), jnp.float32),
                pltpu.VMEM((width // LANES, height + 16, LANES), jnp.float32),
                pltpu.VMEM((3 * LANES, 2 * LANES), jnp.bfloat16),
                pltpu.VMEM((16, LANES), jnp.float32),
                pltpu.VMEM((width // LANES // 2, height, LANES), jnp.float32),
                pltpu.VMEM((width // LANES // 2, height, LANES), jnp.float32),
                pltpu.VMEM((9, LANES), jnp.float32),
                pltpu.VMEM((n, 9, LANES), jnp.float32),
                pltpu.SMEM((2,), jnp.int32),
                pltpu.SemaphoreType.DMA((2,)),
                pltpu.SemaphoreType.DMA,
                pltpu.SemaphoreType.DMA,
                pltpu.SemaphoreType.DMA((2,)),
                pltpu.SemaphoreType.DMA((2, PIECES)),
                pltpu.SemaphoreType.DMA,
                pltpu.SemaphoreType.DMA,
            ],
            compiler_params=pltpu.CompilerParams(collective_id=0, has_side_effects=True, vmem_limit_bytes=room),
        )(*[pltpu.with_memory_space_constraint(x, pltpu.HBM) for x in (bin_index, elevation, ranks)])
        return pl.pallas_call(
            functools.partial(shade_kernel, chunk),
            out_shape=whole,
            in_specs=[inside] * 4,
            out_specs=anywhere,
            scratch_shapes=[block, pltpu.SemaphoreType.DMA],
            compiler_params=pltpu.CompilerParams(vmem_limit_bytes=32 * height * width * 4),
        )(sums, index, slope_x, slope_y)

    in_specs = (P(("groups", "row"), None), P(("groups", "row"), None), P("groups"))
    return jax.shard_map(body, mesh=mesh, in_specs=in_specs, out_specs=P(("groups", "row"), None), check_vma=False)
```

```python
import functools

import jax
import jax.numpy as jnp
from jax import lax
from jax.experimental import pallas as pl
from jax.experimental.pallas import tpu as pltpu
from jax.sharding import PartitionSpec as P

BINS = 1024
zfactor = 200.0
cos_zenith = 0.70710678
sin_zenith = 0.70710678
light_x = -0.70710678
light_y = 0.70710678
LANES = 128
HALO = 4
PAD = 128
SMOOTH = (1.0, 8.0, 28.0, 56.0, 70.0, 56.0, 28.0, 8.0, 1.0)
SLOPE = (-1.0, -6.0, -14.0, -14.0, 0.0, 14.0, 14.0, 6.0, 1.0)
UPPER = 32
LOWER = BINS // UPPER
LEVELS = 255.0
FIELD = 8
PIECES = 2
MESH = pl.DeviceIdType.MESH


def band(first):
    row = lax.broadcasted_iota(jnp.int32, (LANES, LANES), 0)
    col = lax.broadcasted_iota(jnp.int32, (LANES, LANES), 1)
    delta = row + first - col
    rise = jnp.zeros(row.shape, jnp.float32)
    level = jnp.zeros(row.shape, jnp.float32)
    for k in range(9):
        here = delta == k - HALO
        rise = jnp.where(here, SLOPE[k], rise)
        level = jnp.where(here, SMOOTH[k], level)
    return jnp.concatenate([rise, level], axis=1).astype(jnp.bfloat16)


def pick(table, lane):
    numbers = lax.GatherDimensionNumbers(offset_dims=(), collapsed_slice_dims=(1,), start_index_map=(1,),
                                         operand_batching_dims=(0,), start_indices_batching_dims=(0,))
    return lax.gather(table, lane[..., None], numbers, slice_sizes=(1, 1), mode=lax.GatherScatterMode.PROMISE_IN_BOUNDS)


def windows(parts, tiles):
    rows = []
    for t in range(tiles):
        for part in parts:
            rows.append(part[:, t * LANES : (t + 3) * LANES])
    return jnp.concatenate(rows, axis=0)


def target(me, k):
    return k - 1 + (k - 1 >= me).astype(jnp.int32)


def kernel(n, chunk, bins_hbm, elev_hbm, ranks_hbm, sums_ref, bins, slope_x, slope_y, cells, halo, col_x, col_y,
           weights, extremes, high, low, send, recv, ranks, bins_sem, elev_sem, rank_sem, halo_send, halo_recv, send_sem, recv_sem):
    me = lax.axis_index("row")
    height, width = elev_hbm.shape
    chunks = width // chunk
    tiles = chunk // LANES
    inner = pl.ds(PAD, width)
    parts = halo_recv.shape[1]
    piece = width // parts

    def bins_load(half):
        where = (slice(None), pl.ds(pl.multiple_of(half * (width // 2), width // 2), width // 2))
        return pltpu.make_async_copy(bins_hbm.at[where], bins.at[where], bins_sem.at[half])

    elev_load = pltpu.make_async_copy(elev_hbm, cells.at[:, inner], elev_sem)
    rank_load = pltpu.make_async_copy(ranks_hbm, ranks, rank_sem)
    bins_load(0).start()
    bins_load(1).start()
    elev_load.start()
    rank_load.start()

    barrier = pltpu.get_barrier_semaphore()

    def greet(k, carry):
        pl.semaphore_signal(barrier, inc=1, device_id={"row": target(me, k)}, device_id_type=MESH)
        return carry

    lax.fori_loop(1, n, greet, 0)

    for edge in (0, PAD + width):
        cells[:, pl.ds(edge, PAD)] = jnp.zeros((height, PAD), jnp.float32)
        halo[:, pl.ds(edge, PAD)] = jnp.zeros((8, PAD), jnp.float32)

    @pl.when(me == 0)
    def _():
        halo[4:8, inner] = jnp.zeros((4, width), jnp.float32)

    @pl.when(me == n - 1)
    def _():
        halo[0:4, inner] = jnp.zeros((4, width), jnp.float32)

    def halo_copy(way, p):
        rows = pl.ds(0, HALO) if way else pl.ds(height - HALO, HALO)
        cols = pl.ds(PAD + p * piece, piece)
        return pltpu.make_async_remote_copy(
            src_ref=cells.at[rows, cols], dst_ref=halo.at[pl.ds(0 if way else 4, HALO), cols],
            send_sem=halo_send.at[way], recv_sem=halo_recv.at[way, p],
            device_id={"row": lax.rem(me + n - 1, n) if way else lax.rem(me + 1, n)}, device_id_type=MESH)

    urow = lax.broadcasted_iota(jnp.int32, (UPPER, chunk), 0)
    upper_iota = (4 * lax.rem(urow, 8) + urow // 8).astype(jnp.float32).astype(jnp.bfloat16)
    lower_iota = lax.broadcasted_iota(jnp.int32, (LOWER, chunk), 0).astype(jnp.float32).astype(jnp.bfloat16)
    one, zero = jnp.ones((), jnp.bfloat16), jnp.zeros((), jnp.bfloat16)

    def spread(ref, t, r):
        row = jnp.concatenate([ref[t + c, pl.ds(r, 8, stride=0), :] for c in range(tiles)], axis=1)
        return jnp.concatenate([row] * (UPPER // 8), axis=0).astype(jnp.bfloat16)

    def count(half, i, total):
        at = pl.multiple_of((half * (chunks // 2) + i) * chunk, chunk)
        whole = bins[:, pl.ds(at, chunk)]
        for c in range(tiles):
            tile = whole[:, c * LANES : (c + 1) * LANES]
            high[i * tiles + c] = (tile >> 5).astype(jnp.float32)
            low[i * tiles + c] = (tile & 31).astype(jnp.float32)
        for r in range(height):
            hot_u = jnp.where(spread(high, i * tiles, r) <= upper_iota, one, zero).astype(jnp.float8_e4m3fn)
            hot_l = jnp.where(spread(low, i * tiles, r) <= lower_iota, one, zero).astype(jnp.float8_e4m3fn)
            total = total + lax.dot_general(hot_u, hot_l, (((1,), (1,)), ((), ())),
                                            preferred_element_type=jnp.float32)
        return total

    def reach():
        tops, bottoms = [None] * 4, [None] * 4
        for c in range(width // LANES):
            for r in range(height // 8):
                block = cells[8 * r : 8 * r + 8, PAD + c * LANES : PAD + (c + 1) * LANES]
                at = (c * (height // 8) + r) % 4
                tops[at] = block if tops[at] is None else jnp.maximum(tops[at], block)
                bottoms[at] = block if bottoms[at] is None else jnp.minimum(bottoms[at], block)
        extremes[0:8, :] = functools.reduce(jnp.maximum, [x for x in tops if x is not None])
        extremes[8:16, :] = functools.reduce(jnp.minimum, [x for x in bottoms if x is not None])

    def half_count(half, total):
        bins_load(half).wait()
        for i in range(chunks // 2):
            total = count(half, i, total)

        @pl.when(half == 0)
        def _():
            elev_load.wait()
            pl.semaphore_wait(barrier, n - 1)

            @pl.when(me < n - 1)
            def _():
                for p in range(parts):
                    halo_copy(0, p).start()

            @pl.when(me > 0)
            def _():
                for p in range(parts):
                    halo_copy(1, p).start()

            reach()

        return total

    total = lax.fori_loop(0, 2, half_count, jnp.zeros((UPPER, LOWER), jnp.float32))
    counts = jnp.concatenate([total[8 * q : 8 * q + 8] for q in range(UPPER // 8)], axis=1)
    send[0:8, :] = counts
    ends = [jnp.max(extremes[0:8, :], axis=0, keepdims=True), jnp.max(-extremes[8:16, :], axis=0, keepdims=True)]
    top, bottom = [jnp.maximum(x, pltpu.roll(x, LANES // 2, 1)) for x in ends]
    send[8:9, :] = jnp.where(lax.broadcasted_iota(jnp.int32, (1, LANES), 1) < LANES // 2, top, bottom)

    def post(k, carry):
        pltpu.make_async_remote_copy(
            src_ref=send, dst_ref=recv.at[me], send_sem=send_sem, recv_sem=recv_sem,
            device_id={"row": target(me, k)}, device_id_type=MESH).start()
        return carry

    lax.fori_loop(1, n, post, 0)

    for k in range(3):
        weights[k * LANES : (k + 1) * LANES, :] = band((k - 1) * LANES)
    middle = cells[0:1, PAD : PAD + 1]

    def split(x):
        x = x - middle
        first = x.astype(jnp.bfloat16).astype(jnp.float32)
        return first, x - first

    def own_rows(i, carry):
        at = pl.multiple_of(i * chunk, chunk)
        first, rest = split(cells[:, pl.ds(at, chunk + 2 * PAD)])
        got = jnp.dot(windows((first.astype(jnp.bfloat16), rest.astype(jnp.bfloat16)), tiles), weights[...],
                      preferred_element_type=jnp.float32)
        for t in range(tiles):
            both = got[2 * height * t : 2 * height * t + height] + got[2 * height * t + height : 2 * height * (t + 1)]
            col_x[i * tiles + t, 8 : 8 + height, :] = both[:, 0:LANES]
            col_y[i * tiles + t, 8 : 8 + height, :] = both[:, LANES : 2 * LANES]
        return carry

    lax.fori_loop(0, chunks, own_rows, 0, unroll=4)

    def halo_rows(i):
        at = i * chunk
        first, rest = split(halo[:, pl.ds(at, chunk + 2 * PAD)])
        pair = jnp.concatenate([first, rest], axis=0).astype(jnp.bfloat16)
        got = jnp.dot(windows((pair,), tiles), weights[...], preferred_element_type=jnp.float32)
        for t in range(tiles):
            both = got[16 * t : 16 * t + 8] + got[16 * t + 8 : 16 * t + 16]
            for col, lanes in ((col_x, slice(0, LANES)), (col_y, slice(LANES, 2 * LANES))):
                col[i * tiles + t, 0:8, :] = both[:, lanes]
                col[i * tiles + t, 8 + height : 16 + height, :] = both[:, lanes]

    def down_rows(t):
        for r in range(height // 8):
            rows = [col_x[t, 8 * r + 4 + k : 8 * r + 12 + k, :] for k in range(9)]
            out = SMOOTH[4] * rows[4] + (rows[0] + rows[8])
            for k in range(1, 4):
                out = out + SMOOTH[k] * (rows[k] + rows[8 - k])
            slope_x[8 * r : 8 * r + 8, t * LANES : (t + 1) * LANES] = out
            rows = [col_y[t, 8 * r + 4 + k : 8 * r + 12 + k, :] if k != 4 else None for k in range(9)]
            out = 14.0 * ((rows[5] - rows[3]) + (rows[6] - rows[2])) + 6.0 * (rows[7] - rows[1]) + (rows[8] - rows[0])
            slope_y[8 * r : 8 * r + 8, t * LANES : (t + 1) * LANES] = out

    def arrive(p):
        @pl.when(me > 0)
        def _():
            halo_copy(0, p).wait_recv()

        @pl.when(me < n - 1)
        def _():
            halo_copy(1, p).wait_recv()

    arrive(0)
    each = chunks // parts
    for p in range(parts):
        if p + 1 < parts:
            arrive(p + 1)
        for i in range(p * each, (p + 1) * each):
            halo_rows(i)
        for t in range(p * each * tiles, (p + 1) * each * tiles):
            down_rows(t)

    rank_load.wait()
    first, second = ranks[0], ranks[1]
    sums_ref[10:11, :] = jnp.full((1, LANES), first, jnp.int32).astype(jnp.float32)
    sums_ref[11:12, :] = LEVELS / jnp.full((1, LANES), second - first, jnp.int32).astype(jnp.float32)
    recv[me] = send[...]
    edge = halo.at[pl.ds(0, HALO), inner]

    @pl.when(me < n - 1)
    def _():
        pltpu.make_async_copy(edge, edge, halo_send.at[0]).wait()

    @pl.when(me > 0)
    def _():
        pltpu.make_async_copy(edge, edge, halo_send.at[1]).wait()

    everything = recv.at[pl.ds(1, n - 1)]
    pltpu.make_async_copy(everything, everything, send_sem).wait()
    arrivals = pltpu.make_async_copy(everything, everything, recv_sem)
    arrivals.wait()

    def take(k, carry):
        return carry[0] + recv[k, 0:8, :], jnp.maximum(carry[1], recv[k, 8:9, :])

    counts, ends = lax.fori_loop(1, n, take, (recv[0, 0:8, :], recv[0, 8:9, :]), unroll=n <= 16)
    sums_ref[0:8, :] = counts
    sums_ref[8:9, :] = ends


def shade_kernel(chunk, sums_ref, index_ref, slope_x, slope_y, out_ref, result, out_sem):
    height, width = index_ref.shape
    chunks = width // chunk

    counts = sums_ref[0:8, :]
    ends = sums_ref[8:9, :]
    span = (jnp.max(ends[:, 0 : LANES // 2], axis=1, keepdims=True)
            + jnp.max(ends[:, LANES // 2 : LANES], axis=1, keepdims=True))
    scale = jnp.broadcast_to(zfactor / (8.0 * span) * (1.0 / 4096.0), (8, LANES))
    tilt = (sin_zenith * light_y) * scale
    lane = lax.broadcasted_iota(jnp.int32, (8, LANES), 1)
    row = lax.broadcasted_iota(jnp.int32, (8, LANES), 0)
    before = pltpu.roll(counts, LOWER, 1)
    above = jnp.where(row == 0, 0.0, pltpu.roll(before, 1, 0))
    before = jnp.where(lane < LOWER, above, before)
    full = pick(before, lane | (LOWER - 1))
    first = jnp.broadcast_to(sums_ref[10:11, :], (8, LANES))
    steps = jnp.broadcast_to(sums_ref[11:12, :], (8, LANES))
    fixed = jnp.floor(jnp.clip(((full - first) + (counts - before)) * steps, 0.0, LEVELS) + 0.5).astype(jnp.int32)
    spread = [jnp.broadcast_to(fixed[b : b + 1], (8, LANES)) for b in range(8)]
    words = [spread[g] + (spread[g + 1] << FIELD) + (spread[g + 2] << (2 * FIELD)) + (spread[g + 3] << (3 * FIELD))
             for g in (0, 4)]

    def out_copy(i):
        at = pl.multiple_of(i * chunk, chunk)
        where = (slice(None), pl.ds(at, chunk))
        return pltpu.make_async_copy(result.at[where], out_ref.at[where], out_sem)

    def finish(i, carry):
        at = pl.multiple_of(i * chunk, chunk)
        for r in range(height // 8):
            for c in range(chunk // LANES):
                rows = pl.ds(8 * r, 8)
                cols = pl.ds(at + c * LANES, LANES)
                which = index_ref[rows, cols]
                lane = which & (LANES - 1)
                words_at = [pick(w, lane) for w in words]
                word = jnp.where(which >= BINS // 2, words_at[1], words_at[0])
                stretch = ((word >> ((which >> 4) & 24)) & 255).astype(jnp.float32)
                rise, fall = slope_x[rows, cols], slope_y[rows, cols]
                gx, gy = rise * scale, fall * scale
                light = (cos_zenith - tilt * (fall - rise)) * lax.rsqrt(1.0 + gx * gx + gy * gy)
                result[rows, cols] = stretch * (0.5 / LEVELS + (1.0 / LEVELS) * jnp.maximum(light, 0.0))
        out_copy(i).start()
        return carry

    lax.fori_loop(0, chunks, finish, 0, unroll=True)

    pltpu.make_async_copy(result, out_ref, out_sem).wait()


def chunk_of(width):
    chunk = 1024
    while width % chunk:
        chunk //= 2
    return chunk


def solution(mesh):
    n = mesh.shape["row"]

    def body(elevation, bin_index, ranks):
        height, width = elevation.shape
        chunk = chunk_of(width)
        grid = (height, width)
        room = 24 << 20
        block = pltpu.VMEM(grid, jnp.float32)
        whole = jax.ShapeDtypeStruct(grid, jnp.float32)
        anywhere = pl.BlockSpec(memory_space=pl.ANY)
        inside = pl.BlockSpec(memory_space=pltpu.VMEM)
        wide = width + 2 * PAD
        sums, index, slope_x, slope_y = pl.pallas_call(
            functools.partial(kernel, n, chunk),
            out_shape=[jax.ShapeDtypeStruct((16, LANES), jnp.float32), jax.ShapeDtypeStruct(grid, jnp.int32), whole, whole],
            in_specs=[anywhere] * 3,
            out_specs=[inside] * 4,
            scratch_shapes=[
                pltpu.VMEM((height, wide), jnp.float32),
                pltpu.VMEM((8, wide), jnp.float32),
                pltpu.VMEM((width // LANES, height + 16, LANES), jnp.float32),
                pltpu.VMEM((width // LANES, height + 16, LANES), jnp.float32),
                pltpu.VMEM((3 * LANES, 2 * LANES), jnp.bfloat16),
                pltpu.VMEM((16, LANES), jnp.float32),
                pltpu.VMEM((width // LANES // 2, height, LANES), jnp.float32),
                pltpu.VMEM((width // LANES // 2, height, LANES), jnp.float32),
                pltpu.VMEM((9, LANES), jnp.float32),
                pltpu.VMEM((n, 9, LANES), jnp.float32),
                pltpu.SMEM((2,), jnp.int32),
                pltpu.SemaphoreType.DMA((2,)),
                pltpu.SemaphoreType.DMA,
                pltpu.SemaphoreType.DMA,
                pltpu.SemaphoreType.DMA((2,)),
                pltpu.SemaphoreType.DMA((2, PIECES)),
                pltpu.SemaphoreType.DMA,
                pltpu.SemaphoreType.DMA,
            ],
            compiler_params=pltpu.CompilerParams(collective_id=0, has_side_effects=True, vmem_limit_bytes=room),
        )(*[pltpu.with_memory_space_constraint(x, pltpu.HBM) for x in (bin_index, elevation, ranks)])
        return pl.pallas_call(
            functools.partial(shade_kernel, chunk),
            out_shape=whole,
            in_specs=[inside] * 4,
            out_specs=anywhere,
            scratch_shapes=[block, pltpu.SemaphoreType.DMA],
            compiler_params=pltpu.CompilerParams(vmem_limit_bytes=32 * height * width * 4),
        )(sums, index, slope_x, slope_y)

    in_specs = (P(("groups", "row"), None), P(("groups", "row"), None), P("groups"))
    return jax.shard_map(body, mesh=mesh, in_specs=in_specs, out_specs=P(("groups", "row"), None), check_vma=False)
```
